32 devices in a mesh: ctx: 4 (over z), kvh: 4 (over y, x), conv: 2 (over core).
Axes of the slice: x: 2, y: 2, z: 4, core: 2. Of those that a mesh axis runs over, the one named last changes fastest.
Arguments:
- queries: bfloat16 [2, 512, 64, 128], P('conv', 'ctx', 'kvh'), may hold values from -6 to 6
- keys: bfloat16 [2, 4096, 8, 128], P('conv', 'ctx', 'kvh'), may hold values from -6 to 6
- values: bfloat16 [2, 4096, 8, 128], P('conv', 'ctx', 'kvh'), may hold values from -6 to 6
- lengths: int32 [2], P('conv'), may hold values from 64 to 3584
Outputs:
- attended: bfloat16 [2, 512, 64, 128], P('conv', 'ctx', 'kvh')
The draws below stay inside these ranges and needn't reach their ends.
Inputs may be any that keep to these rules, and one draw needn't show every extreme that they name: The new turn's keys and values stand at cache positions lengths to lengths + 511; later positions hold unused entries.
All inputs are finite; a program needn't handle non-finite values.
Results may differ from the reference program's by a relative error of at most 0.005.
Values may be sent and summed in bfloat16 or wider, within the bound.
No kernel may reach another device: no remote copies, remote signals or barrier semaphores. Data moves between devices by JAX's collectives and lax.ppermute only.
A program may use at most 64 MiB of HBM per device.

```python
import jax
import jax.numpy as jnp
from jax import lax

HEADS = 64
KV_HEADS = 8
HEAD_DIM = 128
NEW = 512
CTX_DEV = 1024
CONV_DEV = 1
CTX = 4096
CONV = 2
N_CTX = 4
N_CONV = 2


def draw_queries(key, part):
    shape = (CONV_DEV * N_CONV, NEW, HEADS, HEAD_DIM)
    return jnp.clip(jax.random.normal(jax.random.fold_in(key, 1), shape, jnp.float32), -6.0, 6.0).astype(jnp.bfloat16)


def draw_keys(key, part):
    shape = (CONV_DEV * N_CONV, CTX_DEV * N_CTX, KV_HEADS, HEAD_DIM)
    return jnp.clip(jax.random.normal(jax.random.fold_in(key, 1), shape, jnp.float32), -6.0, 6.0).astype(jnp.bfloat16)


def level_of(own_key, dims, cuts, low, largest):
    factor_of, own = 1.0, jax.random.fold_in(own_key, 6)
    for position, blocks in cuts:
        draws = jnp.exp(jax.random.uniform(jax.random.fold_in(own, position), (blocks,), jnp.float32, low / len(cuts), largest / len(cuts)))
        factor_of = factor_of * jnp.repeat(draws, dims[position] // blocks).reshape([-1 if axis == position else 1 for axis in range(len(dims))])
    return factor_of


def noise(rng, shape, width, reach, shards=(), held_as=jnp.bfloat16):
    level = level_of(rng, shape, shards, -0.22, 0.18) if shards else 1.0
    values = jax.random.normal(rng, shape, jnp.float32) * width * level
    return jnp.minimum(jnp.maximum(values, -reach), reach).astype(held_as)


def setup_inputs(seed: int = 0) -> dict:
    arg_keys = jax.random.split(jax.random.key(seed), 5)
    return {
        "queries": draw_queries(jax.random.fold_in(arg_keys[4], 71), 0),
        "keys": draw_keys(jax.random.fold_in(arg_keys[4], 71), 0),
        "values": noise(arg_keys[2], (CONV, CTX, KV_HEADS, HEAD_DIM), 1.0, 6.0, ((0, 2), (1, 4), (2, 4))),
        "lengths": jax.random.randint(arg_keys[3], (CONV,), 64, CTX_DEV * N_CTX - NEW + 1).astype(jnp.int32),
    }


mask_fill = -1e30


def shard_part(query_float, key_float, value_float, query_position, key_position):
    score_scale = 1.0 / (HEAD_DIM ** 0.5)
    scores = jnp.einsum('tkgd,skd->ktgs', query_float, key_float) * score_scale
    visible = key_position[None, None, None, :] <= query_position[None, :, None, None]
    masked = jnp.where(visible, scores, mask_fill)
    row_max = jnp.max(masked, axis=-1)
    weights = jnp.where(visible, jnp.exp(masked - row_max[..., None]), 0.0)
    exp_total = jnp.sum(weights, axis=-1)
    rounded = weights.astype(jnp.bfloat16)
    weighted = jnp.einsum('ktgs,skd->ktgd', rounded.astype(jnp.float32), value_float)
    safe_total = jnp.maximum(exp_total, 1.0)
    partial_value = (weighted / safe_total[..., None]).astype(jnp.bfloat16)
    log_total = row_max + jnp.log(safe_total)
    return partial_value, log_total


def per_conv(conv_args):
    query_rows, key_rows, value_rows, length = conv_args
    group_size = HEADS // KV_HEADS
    query_float = query_rows.astype(jnp.float32).reshape(NEW, KV_HEADS, group_size, HEAD_DIM)
    query_position = length + jnp.arange(NEW, dtype=jnp.int32)

    def per_shard(shard_index):
        offset = (shard_index * CTX_DEV).astype(jnp.int32)
        key_float = lax.dynamic_slice_in_dim(key_rows, offset, CTX_DEV, 0).astype(jnp.float32)
        value_float = lax.dynamic_slice_in_dim(value_rows, offset, CTX_DEV, 0).astype(jnp.float32)
        key_position = offset + jnp.arange(CTX_DEV, dtype=jnp.int32)
        return shard_part(query_float, key_float, value_float, query_position, key_position)

    partials, log_totals = lax.map(per_shard, jnp.arange(N_CTX, dtype=jnp.int32))
    top = jnp.max(log_totals, axis=0)
    share = jnp.exp(log_totals - top[None])
    numerator = jnp.sum(share[..., None] * partials.astype(jnp.float32), axis=0)
    denominator = jnp.sum(share, axis=0)
    result = (numerator / denominator[..., None]).astype(jnp.bfloat16)
    return jnp.transpose(result, (1, 0, 2, 3)).reshape(NEW, HEADS, HEAD_DIM)


def reference(queries, keys, values, lengths):
    return lax.map(per_conv, (queries, keys, values, lengths))
```

```python
import functools

import jax
import jax.numpy as jnp
from jax import lax
from jax.experimental import pallas as pl
from jax.experimental.pallas import tpu as pltpu
from jax.sharding import PartitionSpec as P

mask_fill = -1e30
empty_max = -1e29
block_rows = 256
tail_rows = 32


def attend_body(where_ref, q_ref, kv_own_ref, kv_next_ref, out_ref, m_ref, l_ref, acc_ref, lse_ref, *, group, exponent_scale, score_scale):
    step = pl.program_id(0)
    rows = m_ref.shape[0]
    lanes = out_ref.shape[1]
    keys = kv_own_ref.shape[1]
    row_tokens = rows // group
    total_rows = rows * pl.num_programs(0)
    first = where_ref[0] + step * row_tokens
    q = q_ref[...].reshape(rows, lanes)
    m_ref[...] = jnp.full(m_ref.shape, empty_max, jnp.float32)
    l_ref[...] = jnp.zeros(l_ref.shape, jnp.float32)
    acc_ref[...] = jnp.zeros(acc_ref.shape, jnp.float32)

    def one_shard(kv_ref, base, masked):
        scores = lax.dot_general(q, kv_ref[0], (((1,), (1,)), ((), ())), preferred_element_type=jnp.float32)
        if masked:
            ahead = lax.broadcasted_iota(jnp.int32, scores.shape, 1) - lax.broadcasted_iota(jnp.int32, scores.shape, 0) // group
            scores = jnp.where(ahead <= first - base, scores, mask_fill)
        old = m_ref[...]
        new = jnp.maximum(old, jnp.max(scores, axis=-1, keepdims=True))
        alpha = jnp.exp2((old - new) * exponent_scale)
        weights = jnp.exp2((scores - new[:, :1]) * exponent_scale).astype(jnp.bfloat16)
        value = kv_ref[1]
        widened = jnp.concatenate([value, jnp.ones_like(value)], axis=1)
        mixed = jnp.dot(weights, widened, preferred_element_type=jnp.float32)
        acc_ref[...] = acc_ref[...] * alpha + mixed[:, :lanes]
        l_ref[...] = l_ref[...] * alpha + mixed[:, lanes:]
        m_ref[...] = new

    for slot, kv_ref in ((1, kv_own_ref), (2, kv_next_ref)):
        base = where_ref[slot]
        full = first >= base + keys - 1
        some = first + row_tokens - 1 >= base

        @pl.when(full)
        def _():
            one_shard(kv_ref, base, False)

        @pl.when(jnp.logical_and(some, jnp.logical_not(full)))
        def _():
            one_shard(kv_ref, base, True)

    total = jnp.maximum(l_ref[...], 1.0)
    out_ref[pl.ds(pl.multiple_of(step * rows, rows), rows), :] = (acc_ref[...] / total).astype(jnp.bfloat16)
    lse = m_ref[...] * score_scale + jnp.log(total)
    diagonal = lax.broadcasted_iota(jnp.int32, (lanes, lanes), 0) == lax.broadcasted_iota(jnp.int32, (lanes, lanes), 1)
    for part in range(rows // lanes):
        piece = jnp.where(diagonal, lse[part * lanes : (part + 1) * lanes], 0.0)
        lse_ref[pl.ds(step * (rows // lanes) + part, 1), :] = jnp.sum(piece, axis=0, keepdims=True)

    @pl.when(step == pl.num_programs(0) - 1)
    def _():
        whole = lse_ref[...]
        high = whole.astype(jnp.bfloat16).astype(jnp.float32)
        middle = (whole - high).astype(jnp.bfloat16).astype(jnp.float32)
        low = whole - high - middle
        tail = jnp.concatenate([high, middle, low, jnp.zeros_like(low)], axis=0)
        out_ref[out_ref.shape[0] - tail.shape[0] :, :] = tail.astype(jnp.bfloat16)


def attend(where, queries, kv_own, kv_next, head, group, name):
    tok_dev, _, head_dim = queries.shape
    keys = kv_own.shape[1]
    total_rows = tok_dev * group
    rows = min(block_rows, total_rows)
    lse_rows = total_rows // head_dim
    body = functools.partial(attend_body, group=group, exponent_scale=1.4426950408889634 / head_dim**0.5, score_scale=1.0 / head_dim**0.5)
    return pl.pallas_call(
        body,
        name=name,
        out_shape=jax.ShapeDtypeStruct((total_rows + 4 * lse_rows, head_dim), jnp.bfloat16),
        grid=(total_rows // rows,),
        in_specs=[
            pl.BlockSpec(memory_space=pltpu.SMEM),
            pl.BlockSpec((rows // group, group, head_dim), lambda i: (i, head, 0)),
            pl.BlockSpec((2, keys, head_dim), lambda i: (0, 0, 0)),
            pl.BlockSpec((2, keys, head_dim), lambda i: (0, 0, 0)),
        ],
        out_specs=pl.BlockSpec((total_rows + 4 * lse_rows, head_dim), lambda i: (0, 0)),
        scratch_shapes=[
            pltpu.VMEM((rows, head_dim), jnp.float32),
            pltpu.VMEM((rows, head_dim), jnp.float32),
            pltpu.VMEM((rows, head_dim), jnp.float32),
            pltpu.VMEM((lse_rows, head_dim), jnp.float32),
        ],
        cost_estimate=pl.CostEstimate(flops=8 * total_rows * keys * head_dim, transcendentals=2 * total_rows * keys, bytes_accessed=3 * total_rows * head_dim * 2),
    )(where, queries, kv_own, kv_next)


def merge_body(inner_ref, own_refs, near_refs, far_refs, out_ref, w_ref, *, group):
    step = pl.program_id(0)
    lanes = out_ref.shape[2]
    rows = own_refs[0][0].shape[0]
    row_tokens = rows // group
    inner = inner_ref[0] > 0
    diagonal = lax.broadcasted_iota(jnp.int32, (lanes, lanes), 0) == lax.broadcasted_iota(jnp.int32, (lanes, lanes), 1)

    def totals(ref):
        parts = ref[...].astype(jnp.float32)
        count = parts.shape[0] // 4
        return parts[:count] + parts[count : 2 * count] + parts[2 * count : 3 * count]

    for head in range(len(own_refs)):
        own, own_tail = own_refs[head]
        near, near_tail = near_refs[head]
        far, far_tail = far_refs[head]
        own_total = totals(own_tail)
        other_total = jnp.where(inner, totals(near_tail), totals(far_tail))
        top = jnp.maximum(own_total, other_total)
        own_share = jnp.exp(own_total - top)
        other_share = jnp.exp(other_total - top)
        w_ref[...] = other_share / (own_share + other_share)
        for part in range(rows // lanes):
            row = w_ref[pl.ds(step * (rows // lanes) + part, 1), :]
            column = jnp.sum(jnp.where(diagonal, row, 0.0), axis=1, keepdims=True)
            span = slice(part * lanes, (part + 1) * lanes)
            mine = own[span, :].astype(jnp.float32)
            other = jnp.where(inner, near[span, :].astype(jnp.float32), far[span, :].astype(jnp.float32))
            mixed = (mine + column * (other - mine)).astype(jnp.bfloat16)
            tokens = lanes // group
            out_ref[part * tokens : (part + 1) * tokens, head * group : (head + 1) * group, :] = mixed.reshape(tokens, group, lanes)


def merge(inner, own, near, far, tok_dev, group):
    heads = len(own)
    head_dim = own[0].shape[1]
    total_rows = tok_dev * group
    rows = min(block_rows, total_rows)
    lse_rows = total_rows // head_dim
    tail = 4 * lse_rows

    def body(inner_ref, *refs):
        pairs = [(refs[2 * i], refs[2 * i + 1]) for i in range(3 * heads)]
        merge_body(inner_ref, pairs[:heads], pairs[heads : 2 * heads], pairs[2 * heads :], refs[-2], refs[-1], group=group)

    specs = [pl.BlockSpec((rows, head_dim), lambda i: (i, 0)), pl.BlockSpec((tail, head_dim), lambda i: (total_rows // tail, 0))]
    operands = [array for array in (*own, *near, *far) for _ in range(2)]
    return pl.pallas_call(
        body,
        name="merge",
        out_shape=jax.ShapeDtypeStruct((tok_dev, heads * group, head_dim), jnp.bfloat16),
        grid=(total_rows // rows,),
        in_specs=[pl.BlockSpec(memory_space=pltpu.SMEM)] + specs * (3 * heads),
        out_specs=pl.BlockSpec((rows // group, heads * group, head_dim), lambda i: (i, 0, 0)),
        scratch_shapes=[pltpu.VMEM((lse_rows, head_dim), jnp.float32)],
    )(inner, *operands)


def line_of_pairs(queries, keys, values, lengths):
    count = lax.axis_size("ctx")
    half = count // 2
    index = lax.axis_index("ctx")
    tok_dev, head_dev, head_dim = queries.shape[1:]
    ctx_dev, kv_dev = keys.shape[1:3]
    group = head_dev // kv_dev
    near_pairs = [(half - 1, half), (half, half - 1)]
    far_pairs = [(0, half), (count - 1, half - 1)]
    far_back = [(half, 0), (half - 1, count - 1)]
    kv_pairs = [(i, i ^ 1) for i in range(count)]
    mine = queries[0]
    near = lax.ppermute(mine, "ctx", near_pairs)
    kv = jnp.stack([jnp.transpose(keys[0], (1, 0, 2)), jnp.transpose(values[0], (1, 0, 2))], axis=1)
    kv_own = [kv[h] for h in range(kv_dev)]
    kv_next = [lax.ppermute(kv_own[0], "ctx", kv_pairs)]
    far = lax.ppermute(mine, "ctx", far_pairs)
    kv_next += [lax.ppermute(kv_own[h], "ctx", kv_pairs) for h in range(1, kv_dev)]

    length = lengths[0]
    bases = [index * ctx_dev, (index ^ 1) * ctx_dev]

    def where(owner):
        return jnp.stack([length + owner * tok_dev, *bases]).astype(jnp.int32)

    near_owner = count - 1 - index
    far_owner = jnp.where(index >= half, 0, count - 1)
    own, near_parts, far_parts = [], [], []
    for h in range(kv_dev):
        near_part = attend(where(near_owner), near, kv_own[h], kv_next[h], h, group, f"near{h}")
        near_parts.append(lax.ppermute(near_part, "ctx", near_pairs))
        far_part = attend(where(far_owner), far, kv_own[h], kv_next[h], h, group, f"far{h}")
        far_parts.append(lax.ppermute(far_part, "ctx", far_back))
        own.append(attend(where(index), mine, kv_own[h], kv_next[h], h, group, f"own{h}"))
    inner = jnp.logical_or(index == half - 1, index == half).astype(jnp.int32).reshape(1)
    return merge(inner, own, near_parts, far_parts, tok_dev, group)[None]


def gathered(queries, keys, values, lengths):
    conv_dev, tok_dev, head_dev, head_dim = queries.shape
    ctx_dev = keys.shape[1]
    kv_dev = keys.shape[2]
    group_size = head_dev // kv_dev
    cycle_size = lax.axis_size("ctx")
    score_scale = 1.0 / head_dim**0.5
    key_position = lax.axis_index("ctx") * ctx_dev + jnp.arange(ctx_dev, dtype=jnp.int32)
    piece_rows = lax.all_gather(queries, "ctx", axis=1, tiled=True)
    row_count = piece_rows.shape[1]
    block_size = 64
    block_total = row_count // block_size
    blocks = jnp.moveaxis(
        piece_rows.reshape(conv_dev, block_total, block_size, head_dev, head_dim), 1, 0
    )

    def one_block(block_args):
        query_block, block_index = block_args
        query_block = query_block.reshape(conv_dev, block_size, kv_dev, group_size, head_dim)
        scores = (
            jnp.einsum("cbkgd,cskd->ckbgs", query_block, keys, preferred_element_type=jnp.float32)
            * score_scale
        )
        query_position = (
            lengths[:, None]
            + block_index * block_size
            + jnp.arange(block_size, dtype=jnp.int32)[None, :]
        )
        visible = key_position[None, None, None, None, :] <= query_position[:, None, :, None, None]
        masked = jnp.where(visible, scores, mask_fill)
        row_max = jnp.max(masked, axis=-1)
        weights = jnp.where(visible, jnp.exp(masked - row_max[..., None]), 0.0)
        exp_total = jnp.sum(weights, axis=-1)
        rounded = weights.astype(jnp.bfloat16)
        weighted = jnp.einsum(
            "ckbgs,cskd->ckbgd", rounded, values, preferred_element_type=jnp.float32
        )
        safe_total = jnp.maximum(exp_total, 1.0)
        partial_value = (weighted / safe_total[..., None]).astype(jnp.bfloat16)
        log_total = row_max + jnp.log(safe_total)
        partial_value = jnp.transpose(partial_value, (0, 2, 1, 3, 4)).reshape(
            conv_dev, block_size, head_dev, head_dim
        )
        log_total = jnp.transpose(log_total, (0, 2, 1, 3)).reshape(conv_dev, block_size, head_dev)
        return (partial_value, log_total)

    partial_value, log_total = lax.map(
        one_block, (blocks, jnp.arange(block_total, dtype=jnp.int32))
    )
    partial_value = jnp.moveaxis(partial_value, 0, 1).reshape(
        conv_dev, row_count, head_dev, head_dim
    )
    log_total = jnp.moveaxis(log_total, 0, 1).reshape(conv_dev, row_count, head_dev)
    arrived = lax.all_to_all(
        partial_value.reshape(conv_dev, cycle_size, tok_dev, head_dev, head_dim),
        "ctx",
        split_axis=1,
        concat_axis=1,
        tiled=True,
    )
    arrived_totals = lax.all_to_all(
        log_total.reshape(conv_dev, cycle_size, tok_dev, head_dev),
        "ctx",
        split_axis=1,
        concat_axis=1,
        tiled=True,
    )
    top = jnp.max(arrived_totals, axis=1)
    share = jnp.exp(arrived_totals - top[:, None])
    numerator = jnp.sum(share[..., None] * arrived.astype(jnp.float32), axis=1)
    denominator = jnp.sum(share, axis=1)
    return (numerator / denominator[..., None]).astype(jnp.bfloat16)


def shards(queries, keys, values, lengths):
    if queries.shape[0] == 1 and lax.axis_size("ctx") == 2 * len(("inner", "outer")):
        return line_of_pairs(queries, keys, values, lengths)
    return gathered(queries, keys, values, lengths)


def solution(mesh):
    in_specs = (
        P("conv", "ctx", "kvh", None),
        P("conv", "ctx", "kvh", None),
        P("conv", "ctx", "kvh", None),
        P("conv"),
    )
    out_specs = P("conv", "ctx", "kvh", None)
    return jax.shard_map(shards, mesh=mesh, in_specs=in_specs, out_specs=out_specs, check_vma=False)
```

```python
import functools

import jax
import jax.numpy as jnp
from jax import lax
from jax.experimental import pallas as pl
from jax.experimental.pallas import tpu as pltpu
from jax.sharding import PartitionSpec as P

mask_fill = -1e30
empty_max = -1e29
log2_e = 1.4426950408889634
kernel_vmem = 20 * 2**20


def identity_mask(lanes):
    return lax.broadcasted_iota(jnp.int32, (lanes, lanes), 0) == lax.broadcasted_iota(jnp.int32, (lanes, lanes), 1)


def owner_of(kind, index, count):
    if kind == "own":
        return index
    if kind == "near":
        return count - 1 - index
    return jnp.where(index >= count // 2, 0, count - 1)


def attend_body(length_ref, q_ref, kv_own_ref, kv_next_ref, out_ref, even_ref, odd_ref, *, kind, head, group, rows, tile, scale, count):
    lanes = out_ref.shape[1]
    keys = kv_own_ref.shape[1]
    tok_dev = q_ref.shape[0]
    total_rows = tok_dev * group
    blocks = total_rows // rows
    row_tokens = rows // group
    index = lax.axis_index("ctx")
    first = length_ref[0] + owner_of(kind, index, count) * tok_dev
    sources = ((kv_own_ref, index * keys), (kv_next_ref, (index ^ 1) * keys))
    scores_refs = (even_ref, odd_ref)
    all_keys = len(sources) * keys
    offset = lax.broadcasted_iota(jnp.int32, (rows, lanes), 0) // group - lax.broadcasted_iota(jnp.int32, (rows, lanes), 1)
    diagonal = identity_mask(lanes)

    def score(block):
        q = q_ref[block * row_tokens : (block + 1) * row_tokens, head * group : (head + 1) * group, :].reshape(rows, lanes)
        top = jnp.full((rows, lanes), empty_max, jnp.float32)
        for slot, (kv_ref, base) in enumerate(sources):
            reach = offset + (first + block * row_tokens - base)
            for start in range(0, keys, tile):
                raw = lax.dot_general(
                    q, kv_ref[0, start : start + tile, :], (((1,), (1,)), ((), ())), preferred_element_type=jnp.float32
                )
                for lane in range(0, tile, lanes):
                    masked = jnp.where(reach >= start + lane, raw[:, lane : lane + lanes], mask_fill)
                    top = jnp.maximum(top, masked)
                    place = slot * keys + start + lane
                    scores_refs[block % 2][:, place : place + lanes] = masked
                yield None
        yield jnp.broadcast_to(jnp.max(top, axis=-1, keepdims=True), (rows, lanes))

    def mix(block, top):
        mixed = None
        for slot, (kv_ref, _) in enumerate(sources):
            pieces = []
            for start in range(slot * keys, (slot + 1) * keys, tile):
                for lane in range(start, start + tile, lanes):
                    weights = jnp.exp2((scores_refs[block % 2][:, lane : lane + lanes] - top) * (scale * log2_e))
                    pieces.append(weights.astype(jnp.bfloat16))
                yield None
            value = kv_ref[1]
            widened = jnp.concatenate([value, jnp.ones_like(value)], axis=1)
            product = jnp.dot(jnp.concatenate(pieces, axis=1), widened, preferred_element_type=jnp.float32)
            mixed = product if mixed is None else mixed + product
        total = jnp.maximum(mixed[:, lanes:], 1.0)
        out_ref[block * rows : (block + 1) * rows, :] = (mixed[:, :lanes] / total).astype(jnp.bfloat16)
        log_total = top * scale + jnp.log(total)
        yield [
            jnp.sum(jnp.where(diagonal, log_total[part : part + lanes], 0.0), axis=0, keepdims=True)
            for part in range(0, rows, lanes)
        ]

    top, totals = None, []
    for block in range(blocks + 1):
        ahead = score(block) if block < blocks else iter(())
        behind = mix(block - 1, top) if block > 0 else iter(())
        running = [ahead, behind]
        last = {}
        while running:
            for stream in list(running):
                try:
                    last[id(stream)] = next(stream)
                except StopIteration:
                    running.remove(stream)
        top = last.get(id(ahead))
        totals += last.get(id(behind), [])
    whole = jnp.concatenate(totals, axis=0)
    high = whole.astype(jnp.bfloat16).astype(jnp.float32)
    middle = (whole - high).astype(jnp.bfloat16).astype(jnp.float32)
    low = whole - high - middle
    tail = jnp.concatenate([high, middle, low, jnp.zeros_like(low)], axis=0)
    out_ref[total_rows:, :] = tail.astype(jnp.bfloat16)


def on_chip(array):
    return pltpu.with_memory_space_constraint(array, pltpu.VMEM)


def attend(length, queries, kv_own, kv_next, kind, head, group, count):
    tok_dev, _, head_dim = queries.shape
    keys = kv_own.shape[1]
    total_rows = tok_dev * group
    rows = min(256, total_rows)
    body = functools.partial(
        attend_body, kind=kind, head=head, group=group, rows=rows, tile=min(256, keys), scale=1.0 / head_dim**0.5, count=count
    )
    vmem = pl.BlockSpec(memory_space=pltpu.VMEM)
    return pl.pallas_call(
        body,
        name=f"{kind}{head}",
        out_shape=pltpu.VMEM((total_rows + 4 * total_rows // head_dim, head_dim), jnp.bfloat16),
        in_specs=[pl.BlockSpec(memory_space=pltpu.SMEM), vmem, vmem, vmem],
        out_specs=vmem,
        scratch_shapes=[pltpu.VMEM((rows, 2 * keys), jnp.float32)] * 2,
        compiler_params=pltpu.CompilerParams(vmem_limit_bytes=kernel_vmem),
        cost_estimate=pl.CostEstimate(
            flops=8 * total_rows * keys * head_dim,
            transcendentals=2 * total_rows * keys,
            bytes_accessed=2 * head_dim * (2 * total_rows + 4 * keys),
        ),
    )(length, on_chip(queries), on_chip(kv_own), on_chip(kv_next))


def merge_body(*refs, heads, group, half):
    own_refs, near_refs, far_refs, out_ref = refs[:heads], refs[heads : 2 * heads], refs[2 * heads : 3 * heads], refs[-1]
    tok_dev, _, lanes = out_ref.shape
    total_rows = tok_dev * group
    count = total_rows // lanes
    index = lax.axis_index("ctx")
    inner = jnp.logical_or(index == half - 1, index == half)
    diagonal = identity_mask(lanes)

    def totals(ref):
        parts = ref[total_rows:, :].astype(jnp.float32)
        return parts[:count] + parts[count : 2 * count] + parts[2 * count : 3 * count]

    def combine(other_refs):
        for head in range(heads):
            own_total = totals(own_refs[head])
            other_total = totals(other_refs[head])
            top = jnp.maximum(own_total, other_total)
            own_share = jnp.exp(own_total - top)
            other_share = jnp.exp(other_total - top)
            portion = other_share / (own_share + other_share)
            for part in range(count):
                column = jnp.sum(jnp.where(diagonal, portion[part : part + 1], 0.0), axis=1, keepdims=True)
                span = slice(part * lanes, (part + 1) * lanes)
                mine = own_refs[head][span, :].astype(jnp.float32)
                other = other_refs[head][span, :].astype(jnp.float32)
                mixed = (mine + column * (other - mine)).astype(jnp.bfloat16)
                tokens = lanes // group
                out_ref[part * tokens : (part + 1) * tokens, head * group : (head + 1) * group, :] = mixed.reshape(tokens, group, lanes)

    @pl.when(inner)
    def _():
        combine(near_refs)

    @pl.when(jnp.logical_not(inner))
    def _():
        combine(far_refs)


def merge(own, near, far, tok_dev, group, half):
    heads = len(own)
    head_dim = own[0].shape[1]
    vmem = pl.BlockSpec(memory_space=pltpu.VMEM)
    return pl.pallas_call(
        functools.partial(merge_body, heads=heads, group=group, half=half),
        name="merge",
        out_shape=jax.ShapeDtypeStruct((tok_dev, heads * group, head_dim), jnp.bfloat16),
        in_specs=[vmem] * (3 * heads),
        out_specs=vmem,
        compiler_params=pltpu.CompilerParams(vmem_limit_bytes=kernel_vmem),
    )(*map(on_chip, (*own, *near, *far)))


def line_of_pairs(queries, keys, values, lengths):
    count = lax.axis_size("ctx")
    half = count // 2
    tok_dev, head_dev, head_dim = queries.shape[1:]
    kv_dev = keys.shape[2]
    group = head_dev // kv_dev
    near_pairs = [(half - 1, half), (half, half - 1)]
    far_pairs = [(0, half), (count - 1, half - 1)]
    far_back = [(half, 0), (half - 1, count - 1)]
    kv_pairs = [(i, i ^ 1) for i in range(count)]
    mine = queries[0]
    near = lax.ppermute(mine, "ctx", near_pairs)
    kv = jnp.stack([jnp.transpose(keys[0], (1, 0, 2)), jnp.transpose(values[0], (1, 0, 2))], axis=1)
    kv_own = [kv[h] for h in range(kv_dev)]
    kv_next = [lax.ppermute(kv_own[0], "ctx", kv_pairs)]
    far = lax.ppermute(mine, "ctx", far_pairs)
    kv_next += [lax.ppermute(kv_own[h], "ctx", kv_pairs) for h in range(1, kv_dev)]
    own, near_parts, far_parts = [], [], []
    for h in range(kv_dev):
        near_part = attend(lengths, near, kv_own[h], kv_next[h], "near", h, group, count)
        near_parts.append(lax.ppermute(near_part, "ctx", near_pairs))
        far_part = attend(lengths, far, kv_own[h], kv_next[h], "far", h, group, count)
        far_parts.append(lax.ppermute(far_part, "ctx", far_back))
        own.append(attend(lengths, mine, kv_own[h], kv_next[h], "own", h, group, count))
    return merge(own, near_parts, far_parts, tok_dev, group, half)[None]


def gathered(queries, keys, values, lengths):
    conv_dev, tok_dev, head_dev, head_dim = queries.shape
    ctx_dev = keys.shape[1]
    kv_dev = keys.shape[2]
    group_size = head_dev // kv_dev
    cycle_size = lax.axis_size("ctx")
    score_scale = 1.0 / head_dim**0.5
    key_position = lax.axis_index("ctx") * ctx_dev + jnp.arange(ctx_dev, dtype=jnp.int32)
    piece_rows = lax.all_gather(queries, "ctx", axis=1, tiled=True)
    row_count = piece_rows.shape[1]
    block_size = 64
    block_total = row_count // block_size
    blocks = jnp.moveaxis(
        piece_rows.reshape(conv_dev, block_total, block_size, head_dev, head_dim), 1, 0
    )

    def one_block(block_args):
        query_block, block_index = block_args
        query_block = query_block.reshape(conv_dev, block_size, kv_dev, group_size, head_dim)
        scores = (
            jnp.einsum("cbkgd,cskd->ckbgs", query_block, keys, preferred_element_type=jnp.float32)
            * score_scale
        )
        query_position = (
            lengths[:, None]
            + block_index * block_size
            + jnp.arange(block_size, dtype=jnp.int32)[None, :]
        )
        visible = key_position[None, None, None, None, :] <= query_position[:, None, :, None, None]
        masked = jnp.where(visible, scores, mask_fill)
        row_max = jnp.max(masked, axis=-1)
        weights = jnp.where(visible, jnp.exp(masked - row_max[..., None]), 0.0)
        exp_total = jnp.sum(weights, axis=-1)
        rounded = weights.astype(jnp.bfloat16)
        weighted = jnp.einsum(
            "ckbgs,cskd->ckbgd", rounded, values, preferred_element_type=jnp.float32
        )
        safe_total = jnp.maximum(exp_total, 1.0)
        partial_value = (weighted / safe_total[..., None]).astype(jnp.bfloat16)
        log_total = row_max + jnp.log(safe_total)
        partial_value = jnp.transpose(partial_value, (0, 2, 1, 3, 4)).reshape(
            conv_dev, block_size, head_dev, head_dim
        )
        log_total = jnp.transpose(log_total, (0, 2, 1, 3)).reshape(conv_dev, block_size, head_dev)
        return (partial_value, log_total)

    partial_value, log_total = lax.map(
        one_block, (blocks, jnp.arange(block_total, dtype=jnp.int32))
    )
    partial_value = jnp.moveaxis(partial_value, 0, 1).reshape(
        conv_dev, row_count, head_dev, head_dim
    )
    log_total = jnp.moveaxis(log_total, 0, 1).reshape(conv_dev, row_count, head_dev)
    arrived = lax.all_to_all(
        partial_value.reshape(conv_dev, cycle_size, tok_dev, head_dev, head_dim),
        "ctx",
        split_axis=1,
        concat_axis=1,
        tiled=True,
    )
    arrived_totals = lax.all_to_all(
        log_total.reshape(conv_dev, cycle_size, tok_dev, head_dev),
        "ctx",
        split_axis=1,
        concat_axis=1,
        tiled=True,
    )
    top = jnp.max(arrived_totals, axis=1)
    share = jnp.exp(arrived_totals - top[:, None])
    numerator = jnp.sum(share[..., None] * arrived.astype(jnp.float32), axis=1)
    denominator = jnp.sum(share, axis=1)
    return (numerator / denominator[..., None]).astype(jnp.bfloat16)


def shards(queries, keys, values, lengths):
    if queries.shape[0] == 1 and lax.axis_size("ctx") == 2 * len(("inner", "outer")):
        return line_of_pairs(queries, keys, values, lengths)
    return gathered(queries, keys, values, lengths)


def solution(mesh):
    in_specs = (
        P("conv", "ctx", "kvh", None),
        P("conv", "ctx", "kvh", None),
        P("conv", "ctx", "kvh", None),
        P("conv"),
    )
    out_specs = P("conv", "ctx", "kvh", None)
    return jax.shard_map(shards, mesh=mesh, in_specs=in_specs, out_specs=out_specs, check_vma=False)
```
